32 devices in a mesh: dp: 4 (over y, core), seq: 2 (over x), expert: 4 (over z).
Axes of the slice: x: 2, y: 2, z: 4, core: 2. Of those that a mesh axis runs over, the one named last changes fastest.
Arguments:
- queries: bfloat16 [512, 4096], P(('dp', 'seq'), 'expert'), parts along dimension 0, may hold values from -256 to 256, as said below
- keys: bfloat16 [2048, 1024], P(('dp', 'seq'), 'expert'), parts along dimension 0, may hold values from -6 to 6
- values: bfloat16 [2048, 1024], P(('dp', 'seq'), 'expert'), parts along dimension 0, may hold values from -6 to 6
- lengths: int32 [32], P('dp'), parts along dimension 0, may hold values from 1 to 256, 512 in all
- routes: int32 [512, 2], P(('dp', 'seq', 'expert')), parts along dimension 0, may hold values from 0 to 3, all different within a row; in each aligned block of 16 rows (0 to 15, 16 to 31, ...) at most 12 rows name the same one
- gates: float32 [512, 2], P(('dp', 'seq', 'expert')), parts along dimension 0, may hold values from 0.2 to 1
- w_up: bfloat16 [4, 4096, 7168], P('expert', None, 'seq'), may hold values from -0.09375 to 0.09375
Outputs:
- expert_mix: bfloat16 [512, 7168], P(('dp', 'seq', 'expert')), parts along dimension 0
The draws below stay inside these ranges and needn't reach their ends.
There are 4 independent parts, one for each index of `dp`. The reference program is written for one: setup_inputs(seed, part) draws one part's arguments, and reference() takes and returns one part's arrays. A program takes and returns all parts, laid end to end along the dimension named above; an argument that names none is the same for every part. Nothing has to cross between parts.
Inputs may be any that keep to these rules, and one draw needn't show every extreme that they name: `queries`: A query row's values are those of a normal draw or, in some rows, a multiple of a sum of key rows. The 8 lengths sum to 512. `routes`: A row's two experts differ; among the 16 rows of one device no expert is named more than 12 times.
All inputs are finite; a program needn't handle non-finite values.
Results may differ from the reference program's by a relative error of at most 0.012.
Values may be sent and summed in bfloat16 or wider, within the bound.
A program may use at most 64 MiB of HBM per device.

```python
import math
import jax
import jax.numpy as jnp
import numpy as np
from jax import lax

D = 4096
H = 32
KVH = 8
HD = 128
EXPERTS = 4
FFW = 7168
SHARD = 256
Q_DEV = 64
NDOC = 8
LEN = 512
QTOK = 128
T_DEV = 16
CAP = 12


def base_keys(key):
    return jnp.clip(jax.random.normal(jax.random.fold_in(key, 71), (LEN, KVH * HD), jnp.float32), -6.0, 6.0)


def draw_keys(key, part):
    return base_keys(key).astype(jnp.bfloat16)


def draw_queries(key, part):
    drawn = jnp.clip(jax.random.normal(jax.random.fold_in(key, 72), (QTOK, H * HD), jnp.float32), -6.0, 6.0)
    return drawn.astype(jnp.bfloat16)


def block_levels(rng, dims, cuts, low, high):
    def one(axis_at, parts):
        heights = jax.random.uniform(jax.random.fold_in(jax.random.fold_in(rng, 6), axis_at), (parts,), jnp.float32, low / len(cuts), high / len(cuts))
        return jnp.repeat(jnp.exp(heights), dims[axis_at] // parts).reshape((-1,) + (1,) * (len(dims) - axis_at - 1))

    level = one(*cuts[0])
    for cut in cuts[1:]:
        level = level * one(*cut)
    return level


def profile(number_of, total, bound, lean):
    loads = [(1 << 20) // math.isqrt(rank ** lean) + 1 for rank in range(2, number_of + 1)]
    surplus, counts = total - bound - (number_of - 1), [1] * (number_of - 1)
    while surplus > 0:
        free = [i for i in range(number_of - 1) if counts[i] < bound]
        pool, budget = sum([loads[i] for i in free]), surplus
        for i in free:
            extra = min(bound - counts[i], max(1, budget * loads[i] // pool), surplus)
            counts[i] = counts[i] + extra
            surplus = surplus - extra
    return np.array([bound] + counts)


def ragged_sizes(own_key, number_of, total, limit, lean):
    if number_of == 2:
        one = jax.random.randint(own_key, (), max(1, total - limit), min(limit, total - 1) + 1)
        return jnp.stack([one, total - one])
    sizes = jnp.asarray(profile(number_of, total, limit, lean), jnp.int32)
    pairs = (number_of - 1) // 2
    giver, receiver = sizes[1:1 + 2 * pairs:2], sizes[2:2 + 2 * pairs:2]
    room = jnp.minimum(giver - 1, limit - receiver)
    moved = jax.random.randint(jax.random.fold_in(own_key, 1), (pairs,), 0, 1 << 20) % (room + 1)
    sizes = sizes.at[1:1 + 2 * pairs:2].set(giver - moved).at[2:2 + 2 * pairs:2].set(receiver + moved)
    return sizes[jax.random.permutation(jax.random.fold_in(own_key, 2), number_of)]


def deal_out(own_key, own, number, rows, number_of, top, bound, skew):
    sequence = jax.random.permutation(own_key, number_of)
    crowded, common = shares(number_of, rows * top, bound, skew, True), shares(number_of, rows * top, bound, skew, False)
    places = jnp.arange(number_of)

    def named(tallies, turn):
        used = int((tallies > 0).sum())
        fixed = max(1, used // 4)
        passed = fixed + (places - fixed + turn * (used - fixed)) % max(1, number_of - fixed)
        return jnp.zeros((number_of,), jnp.int32).at[sequence[jnp.where(places < fixed, places, passed)]].set(jnp.asarray(tallies, jnp.int32))

    tallies = jnp.where(number % 4 == 0, named(crowded, number // 4), named(common, number - number // 4 - 1))
    mixed = jax.random.permutation(jax.random.fold_in(own, 3), number_of)
    donor, receiver = mixed[0:number_of // 2 * 2:2], mixed[1:number_of // 2 * 2:2]
    room = jnp.minimum(tallies[donor] - 1, bound - tallies[receiver]) // 2
    room = jnp.where((donor == sequence[0]) | (receiver == sequence[0]) | (tallies[receiver] == 0), 0, jnp.maximum(room, 0))
    passed = jax.random.randint(jax.random.fold_in(own, 4), (number_of // 2,), 0, 1 << 20) % (room + 1)
    tallies = tallies.at[donor].add(-passed).at[receiver].add(passed)
    members = jnp.searchsorted(jnp.cumsum(tallies), jnp.arange(rows * top), side="right").astype(jnp.int32)
    listing = members.reshape(top, rows).T
    listing = listing[jax.random.permutation(jax.random.fold_in(own, 1), rows)]
    turn = jax.random.randint(jax.random.fold_in(own, 2), (rows, 1), 0, top)
    return jnp.take_along_axis(listing, (jnp.arange(top)[None, :] + turn) % top, axis=1)


def shares(amount, total, limit, skew, full):
    weights = [(1 << 20) // math.isqrt(standing ** skew) + 1 for standing in range(1, amount + 1)]
    largest = limit if full else min(limit, max(-(-total // amount), total * weights[0] // sum(weights)))
    least = 1 if total - largest >= amount - 1 else 0
    given, rest = [largest] + [least] * (amount - 1), total - largest - least * (amount - 1)
    while rest > 0:
        free = [i for i in range(1, amount) if given[i] < largest] or [i for i in range(1, amount) if given[i] < limit]
        whole, left = sum([weights[i] for i in free]), rest
        for i in free:
            extra = min(limit - given[i], max(1, left * weights[i] // whole), rest)
            given[i] = given[i] + extra
            rest = rest - extra
    return np.array(given)


def normal_values(key, shape, scale, bound, pieces=(), held_as=jnp.bfloat16):
    array = jax.random.normal(key, shape, jnp.float32) * scale
    if len(pieces) > 0:
        array = block_levels(key, shape, pieces, -0.22, 0.18) * array
    return jnp.clip(array, min=-bound, max=bound).astype(held_as)


def setup_inputs(seed: int = 0, part: int = 0) -> dict:
    key_of = jax.random.split(jax.random.key(seed), 8)
    part_splits = jax.random.split(jax.random.fold_in(key_of[7], part), 8)
    queries = draw_queries(jax.random.fold_in(jax.random.fold_in(key_of[7], part), 71), part)
    keys = draw_keys(jax.random.fold_in(jax.random.fold_in(key_of[7], part), 71), part)
    values = normal_values(part_splits[2], (LEN, KVH * HD), 1.0, 6.0, ((0, 2), (1, 4)))
    lengths = ragged_sizes(part_splits[3], NDOC, LEN, LEN // 2, 2).astype(jnp.int32)
    routes_keys = jax.random.split(jax.random.fold_in(part_splits[4], 1), QTOK // T_DEV)
    routes_turns = jax.random.permutation(jax.random.fold_in(part_splits[4], 3), QTOK // T_DEV)
    routes = jax.vmap(lambda own, number: deal_out(jax.random.fold_in(part_splits[4], 2), own, number, T_DEV, EXPERTS, 2, CAP, 2))(routes_keys, routes_turns).reshape((QTOK, 2))
    gates = jnp.clip(0.2 + 0.8 * jax.random.uniform(part_splits[5], (QTOK, 2), jnp.float32) ** block_levels(part_splits[5], (QTOK, 2), ((0, 8),), -0.2, 0.2), 0.2, 1.0)
    w_up = normal_values(key_of[6], (EXPERTS, D, FFW), D ** -0.5, 0.09375, ((0, 4), (2, 2)))
    return {"queries": queries, "keys": keys, "values": values, "lengths": lengths, "routes": routes, "gates": gates, "w_up": w_up}


def doc_index(positions, starts):
    return lax.optimization_barrier(jnp.sum((positions[:, None] >= starts[None, :]).astype(jnp.int32), axis=1)) - 1

def reference(queries, keys, values, lengths, routes, gates, w_up):
    qtok = queries.shape[0]
    rows = jnp.arange(qtok, dtype=jnp.int32)
    qpos = rows // Q_DEV * SHARD + SHARD - Q_DEV + rows % Q_DEV
    starts = (jnp.cumsum(lengths) - lengths).astype(jnp.int32)
    kpos = jnp.arange(LEN, dtype=jnp.int32)
    qdoc = doc_index(qpos, starts)
    kdoc = doc_index(kpos, starts)
    allowed = (kpos[None, :] <= qpos[:, None]) & (kdoc[None, :] == qdoc[:, None])
    group = H // KVH
    scale = 1.0 / HD ** 0.5
    q_heads = queries.astype(jnp.float32).reshape(qtok, KVH, group, HD).transpose(1, 2, 0, 3)
    k_heads = keys.astype(jnp.float32).reshape(LEN, KVH, HD).transpose(1, 0, 2)
    v_heads = values.astype(jnp.float32).reshape(LEN, KVH, HD).transpose(1, 0, 2)

    def one_head(operands):
        q_part, k_part, v_part = operands
        score = jnp.einsum('gqd,pd->gqp', q_part, k_part) * scale
        masked = jnp.where(allowed[None], score, jnp.float32(-1e+30))
        peak = lax.optimization_barrier(jnp.max(masked, axis=-1, keepdims=True))
        weight = jnp.where(allowed[None], jnp.exp(score - peak), jnp.float32(0.0))
        total = lax.optimization_barrier(jnp.sum(weight, axis=-1))
        weight_b = lax.optimization_barrier(weight.astype(jnp.bfloat16)).astype(jnp.float32)
        attended = jnp.einsum('gqp,pd->gqd', weight_b, v_part) / total[..., None]
        return attended.astype(jnp.bfloat16)
    heads_out = lax.map(one_head, (q_heads, k_heads, v_heads))
    attended = heads_out.transpose(2, 0, 1, 3).reshape(qtok, H * HD)
    feats = attended.astype(jnp.float32)
    normed = (feats * lax.rsqrt(lax.optimization_barrier(jnp.mean(feats * feats, axis=-1, keepdims=True)) + 1e-05)).astype(jnp.bfloat16)

    def per_expert(acc, operands):
        weight_e, which = operands
        upper = jnp.dot(normed, weight_e, preferred_element_type=jnp.float32)
        act = lax.optimization_barrier(jax.nn.silu(upper).astype(jnp.bfloat16)).astype(jnp.float32)
        share = lax.optimization_barrier(jnp.sum(jnp.where(routes == which, gates, jnp.float32(0.0)), axis=1))
        return (acc + share[:, None] * act, None)
    start_acc = jnp.zeros((qtok, FFW), jnp.float32)
    mixed, _ = lax.scan(per_expert, start_acc, (w_up, jnp.arange(EXPERTS, dtype=jnp.int32)))
    return mixed.astype(jnp.bfloat16)
```

```python
import functools

import jax
import jax.numpy as jnp
from jax import lax
from jax.experimental import pallas as pl
from jax.experimental.pallas import tpu as pltpu
from jax.sharding import PartitionSpec as P

HD = 128
MESH = pl.DeviceIdType.MESH
F32 = jnp.float32
BF16 = jnp.bfloat16
NT = (((1,), (1,)), ((), ()))


def up(n, m):
    return -(-n // m) * m


def iota(shape, dim):
    return lax.broadcasted_iota(jnp.int32, shape, dim)


def onehot(mask):
    return jnp.where(mask, F32(1.0), F32(0.0)).astype(BF16)


def dot(a, b):
    return jnp.dot(a, b, preferred_element_type=F32)


def kernel(
    cfg,
    len_ref, q_ref, k_ref, v_ref, routes_ref, gates_ref, w_hbm, out_ref,
    wbuf, kbuf, vbuf, rbuf, pack, xbuf, acc, sendbuf, recv,
    w_sem, kv_send, kv_recv, r_send, r_recv, z_send, z_recv, x_send, x_recv,
    own_sem, b_send, b_recv,
):
    S, E, ndoc, cap, RB, F, RP, nc, steps, pieces, tile = cfg
    s = lax.axis_index("seq")
    e = lax.axis_index("expert")
    q_rows, width = q_ref.shape
    shard = k_ref.shape[0]
    kvl = k_ref.shape[1] // HD
    group = width // HD // kvl
    T = routes_ref.shape[0]
    ff = w_hbm.shape[1]
    depth = w_hbm.shape[0]
    scale = 1.0 / HD**0.5
    rows = S * RB

    def at_s(d):
        return lax.rem(s + S - d, S)

    def at_e(d):
        return lax.rem(e + E - d, E)

    barrier = pltpu.get_barrier_semaphore()
    for ds in range(S):
        for de in range(E):
            if ds or de:
                pl.semaphore_signal(
                    barrier, inc=1, device_id={"seq": at_s(ds), "expert": at_e(de)},
                    device_id_type=MESH,
                )

    def w_copy(r):
        src = lax.rem(e + r, E)
        return pltpu.make_async_copy(
            w_hbm.at[pl.ds(pl.multiple_of(src * width, width), width)], wbuf.at[r], w_sem.at[r]
        )

    for r in range(E):
        w_copy(r).start()
    pl.semaphore_wait(barrier, S * E - 1)

    def remote(src, dst, ssem, rsem, ds, de):
        return pltpu.make_async_remote_copy(
            src_ref=src, dst_ref=dst, send_sem=ssem, recv_sem=rsem,
            device_id={"seq": at_s(ds), "expert": at_e(de)}, device_id_type=MESH,
        )

    kv_copies = []
    offset = 0
    for i, (d, first) in enumerate(pieces):
        n = shard - first
        kc = remote(k_ref.at[pl.ds(first, n)], kbuf.at[pl.ds(offset, n)],
                    kv_send.at[2 * i], kv_recv.at[2 * i], S - d, 0)
        vc = remote(v_ref.at[pl.ds(first, n)], vbuf.at[pl.ds(offset, n)],
                    kv_send.at[2 * i + 1], kv_recv.at[2 * i + 1], S - d, 0)
        kc.start()
        vc.start()
        kv_copies += [kc, vc]
        offset += n
    r_copies = []
    for de in range(1, E):
        c = remote(routes_ref, rbuf.at[de], r_send.at[de], r_recv.at[de], 0, de)
        c.start()
        r_copies.append(c)

    qn = group * q_rows
    qpos = s * shard + shard - q_rows + lax.rem(iota((qn, 1), 0), q_rows)
    docstart = jnp.zeros((qn, 1), jnp.int32)
    begin = jnp.int32(0)
    for j in range(ndoc):
        docstart = jnp.where(qpos >= begin, begin, docstart)
        begin = begin + len_ref[j]

    def masked(q, k, first):
        sc = lax.dot_general(q, k, NT, preferred_element_type=F32) * scale
        kpos = first + iota((1, k.shape[0]), 1)
        return jnp.where((kpos <= qpos) & (kpos >= docstart), sc, F32(-1e30))

    queries = []
    local = []
    for h in range(kvl):
        q = jnp.concatenate(
            [q_ref[:, (h * group + g) * HD:(h * group + g + 1) * HD] for g in range(group)], axis=0
        )
        queries.append(q)
        local.append(masked(q, k_ref[:, h * HD:(h + 1) * HD], s * shard))

    for c in r_copies:
        c.wait()
    lanes = iota((1, 128), 1)
    mine = routes_ref[...]

    def members(rt):
        return onehot((rt[:, 0:1] == lanes) | (rt[:, 1:2] == lanes))

    eye = onehot(iota((up(E, 8), 128), 0) == iota((up(E, 8), 128), 1))
    upper = onehot(iota((T, T), 0) < iota((T, T), 1))
    blocks = []
    for de in range(E):
        m = members(mine if de == 0 else rbuf[de])
        mt = lax.dot_general(eye, m, NT, preferred_element_type=F32)
        cnt = dot(mt.astype(BF16), upper)
        blk = lax.rem(e + de, E)
        place = jnp.where(mt > 0.5, cnt + (blk * cap).astype(F32), F32(-1.0))
        blocks.append((place, blk))
    Q = q_rows
    total_place = jnp.zeros((up(E, 8), Q), F32)
    for place, blk in blocks:
        shift = onehot(iota((T, Q), 0) + blk * T == iota((T, Q), 1))
        total_place = total_place + dot((place + 1.0).astype(BF16), shift)
    row_of = iota((RB, Q), 0).astype(F32) + 1.0
    sel = []
    for x in range(E):
        sel.append(onehot(total_place[x:x + 1, :] == row_of))
    selector = jnp.concatenate(sel, axis=0)

    for c in kv_copies:
        c.wait()
    for h in range(kvl):
        q = queries[h]
        hs = slice(h * HD, (h + 1) * HD)
        parts = [(local[h], v_ref[:, hs])]
        offset = 0
        for d, first in pieces:
            n = shard - first
            parts.append((masked(q, kbuf[offset:offset + n, hs], (s - d) * shard + first),
                          vbuf[offset:offset + n, hs]))
            offset += n
        peak = jnp.max(parts[0][0], axis=-1, keepdims=True)
        for sc, _ in parts[1:]:
            peak = jnp.maximum(peak, jnp.max(sc, axis=-1, keepdims=True))
        total, got = None, None
        for sc, v in parts:
            wt = jnp.exp(sc - peak)
            t = jnp.sum(wt, axis=-1, keepdims=True)
            o = dot(wt.astype(BF16), v)
            total = t if total is None else total + t
            got = o if got is None else got + o
        att = (got / total).astype(BF16)
        for g in range(group):
            cols = slice((h * group + g) * HD, (h * group + g + 1) * HD)
            packed = dot(selector, att[g * q_rows:(g + 1) * q_rows]).astype(BF16)
            for x in range(E):
                pack[x, :, cols] = packed[x * RB:(x + 1) * RB]

    mine_rows = pl.ds(pl.multiple_of(s * RB, RB), RB)

    z_copies = [None]
    for r in range(1, E):
        c = remote(pack.at[at_e(r)], xbuf.at[r, mine_rows], z_send.at[r], z_recv.at[r], 0, r)
        c.start()
        z_copies.append(c)
    x_copies = []
    for ds in range(1, S):
        c = remote(pack.at[e], xbuf.at[0, mine_rows], x_send.at[0, ds], x_recv.at[0, ds], ds, 0)
        c.start()
        x_copies.append(c)
    own = pltpu.make_async_copy(pack.at[e], xbuf.at[0, mine_rows], own_sem.at[0])
    own.start()

    rows_out, rows_in = E * S * RP, F * rows
    out_row = iota((rows_out, 1), 0)
    inner = lax.rem(out_row, RP)
    which = lax.div(out_row, RP)
    ds_of = lax.rem(which, S)
    de_of = lax.div(which, S)
    f_of = lax.div(inner, cap)
    slot_of = lax.rem(inner, cap)
    s_of = lax.rem(s + S - ds_of, S)
    e_of = lax.rem(e + E - de_of, E)
    from_row = f_of * rows + s_of * RB + e_of * cap + slot_of
    from_row = jnp.where(inner < F * cap, from_row, -1)
    perm = onehot(from_row == iota((rows_out, rows_in), 1))

    m_own = members(mine)
    before = dot(onehot(iota((T, T), 1) < iota((T, T), 0)), m_own)
    picks = []
    wide = iota((T, E * RP), 1)
    at = []
    for k in range(2):
        rk = mine[:, k:k + 1]
        slot = jnp.sum(jnp.where(rk == lanes, before, F32(0.0)), axis=1, keepdims=True)
        rel = rk - e
        rel = jnp.where(rel < 0, rel + E, rel)
        at.append(rel * RP + slot.astype(jnp.int32))
    for f in range(F):
        for k in range(2):
            picks.append(onehot(at[k] + f * cap == wide))
    pick = jnp.concatenate(picks, axis=0)

    square = jnp.zeros((rows, 1), F32)
    sends = []
    for r in range(E):
        if r + 1 < E:
            z_copies[r + 1].wait()
            for ds in range(1, S):
                c = remote(xbuf.at[r + 1, mine_rows], xbuf.at[r + 1, mine_rows],
                           x_send.at[r + 1, ds], x_recv.at[r + 1, ds], ds, 0)
                c.start()
                x_copies.append(c)
        if r == 0:
            own.wait()
        for c in x_copies[r * (S - 1):(r + 1) * (S - 1)]:
            c.wait()
        w_copy(r).wait()
        x = xbuf[r]
        xf = x.astype(F32)
        square = square + jnp.sum(xf * xf, axis=-1, keepdims=True)
        if r < E - 1:
            def body(i, carry, r=r, x=x):
                cols = pl.ds(pl.multiple_of(i * tile, tile), tile)
                part = dot(x, wbuf[r, :, cols])
                if r == 0:
                    acc[:, cols] = part
                else:
                    acc[:, cols] += part
                return carry

            lax.fori_loop(0, ff // tile, body, 0)
        else:
            factor = lax.rsqrt(square / depth + 1e-05)
            for st, (c0, n) in enumerate(steps):
                folded = []
                for f in range(F):
                    cols = slice(f * nc + c0, f * nc + c0 + n)
                    part = dot(x, wbuf[r, :, cols])
                    if r > 0:
                        part = part + acc[:, cols]
                    part = part * factor
                    folded.append((part / (1.0 + jnp.exp(-part))).astype(BF16))
                moved = dot(perm, jnp.concatenate(folded, axis=0)).astype(BF16)
                for de in reversed(range(E)):
                    for ds in reversed(range(S)):
                        base = (de * S + ds) * RP
                        block = moved[base:base + RP]
                        if ds or de:
                            sendbuf[de, ds, :, c0:c0 + n] = block
                        else:
                            recv[0, 0, :, c0:c0 + n] = block
                for de in reversed(range(E)):
                    for ds in reversed(range(S)):
                        if ds or de:
                            c = remote(sendbuf.at[de, ds, :, pl.ds(c0, n)],
                                       recv.at[ds, de, :, pl.ds(c0, n)],
                                       b_send.at[st, de, ds], b_recv.at[st, de, ds], ds, de)
                            c.start()
                            sends.append((st, ds, c))

    g0, g1 = gates_ref[:, 0:1], gates_ref[:, 1:2]
    for st, (c0, n) in enumerate(steps):
        for ds in range(S):
            for a, b, c in sends:
                if a == st and b == ds:
                    c.wait()
            got = recv[ds, :, :, c0:c0 + n].reshape(E * RP, n)
            res = dot(pick, got)
            base = lax.rem(s + ds, S) * ff
            for f in range(F):
                lo = 2 * f * T
                mix = g0 * res[lo:lo + T] + g1 * res[lo + T:lo + 2 * T]
                cols = pl.ds(pl.multiple_of(base + (f * nc + c0), 128), n)
                out_ref[:, cols] = mix.astype(BF16)


def shards(queries, keys, values, lengths, routes, gates, w_up):
    S, E = lax.axis_size("seq"), lax.axis_size("expert")
    q_rows, width = queries.shape
    shard = keys.shape[0]
    w = w_up.reshape(w_up.shape[1], w_up.shape[2])
    depth, ff = w.shape
    T = routes.shape[0]
    cap = max(2, 3 * q_rows // (E * E))
    RB = up(E * cap, 16)
    choices = [f for f in range(1, ff // 128 + 1) if ff % (f * 128) == 0]
    F = min(choices, key=lambda f: up(f * cap, 16) * (ff // f))
    RP = up(F * cap, 16)
    nc = ff // F
    half = up(nc // 2, 256)
    steps = [(0, nc)] if half >= nc else [(0, half), (half, nc - half)]
    tile = 512 if ff % 512 == 0 else 128
    window = shard * S // 2
    pieces = []
    for d in range(1, S):
        first = max(0, (d + 1) * shard - q_rows - window + 1) // 16 * 16
        if first < shard:
            pieces.append((d, first))
    kv_rows = sum(shard - first for _, first in pieces)
    cfg = (S, E, lengths.shape[0], cap, RB, F, RP, nc, steps, pieces, tile)
    vmem = pl.BlockSpec(memory_space=pltpu.VMEM)
    dma = pltpu.SemaphoreType.DMA
    return pl.pallas_call(
        functools.partial(kernel, cfg),
        out_shape=jax.ShapeDtypeStruct((T, S * ff), BF16),
        in_specs=[pl.BlockSpec(memory_space=pltpu.SMEM), vmem, vmem, vmem, vmem, vmem,
                  pl.BlockSpec(memory_space=pl.ANY)],
        out_specs=vmem,
        scratch_shapes=[
            pltpu.VMEM((E, width, ff), BF16),
            pltpu.VMEM((kv_rows, keys.shape[1]), BF16),
            pltpu.VMEM((kv_rows, keys.shape[1]), BF16),
            pltpu.VMEM((E, T, 2), jnp.int32),
            pltpu.VMEM((E, RB, width), BF16),
            pltpu.VMEM((E, S * RB, width), BF16),
            pltpu.VMEM((S * RB, ff), F32),
            pltpu.VMEM((E, S, RP, nc), BF16),
            pltpu.VMEM((S, E, RP, nc), BF16),
            dma((E,)),
            dma((2 * len(pieces),)),
            dma((2 * len(pieces),)),
            dma((E,)), dma((E,)), dma((E,)), dma((E,)),
            dma((E, S)), dma((E, S)),
            dma((1,)),
            dma((len(steps), E, S)), dma((len(steps), E, S)),
        ],
        compiler_params=pltpu.CompilerParams(
            collective_id=0, has_side_effects=True, vmem_limit_bytes=60 * 1024 * 1024
        ),
    )(lengths, queries, keys, values, routes, gates, w)


def solution(mesh):
    placed = (
        P(("dp", "seq"), "expert"),
        P(("dp", "seq"), "expert"),
        P(("dp", "seq"), "expert"),
        P("dp"),
        P(("dp", "seq", "expert"), None),
        P(("dp", "seq", "expert"), None),
        P("expert", None, "seq"),
    )
    return jax.shard_map(
        shards,
        mesh=mesh,
        in_specs=placed,
        out_specs=P(("dp", "seq", "expert"), None),
        check_vma=False,
    )
```

```python
import functools

import jax
import jax.numpy as jnp
from jax import lax
from jax.experimental import pallas as pl
from jax.experimental.pallas import tpu as pltpu
from jax.sharding import PartitionSpec as P

HD = 128
MESH = pl.DeviceIdType.MESH
F32 = jnp.float32
BF16 = jnp.bfloat16
NT = (((1,), (1,)), ((), ()))


def up(n, m):
    return -(-n // m) * m


def iota(shape, dim):
    return lax.broadcasted_iota(jnp.int32, shape, dim)


def onehot(mask):
    return jnp.where(mask, F32(1.0), F32(0.0)).astype(BF16)


def dot(a, b):
    return jnp.dot(a, b, preferred_element_type=F32)


def kernel(
    cfg,
    len_ref, q_ref, k_ref, v_ref, routes_ref, gates_ref, w_hbm, out_ref,
    wbuf, kbuf, vbuf, rbuf, pack, xbuf, acc, sendbuf, recv,
    w_sem, kv_send, kv_recv, r_send, r_recv, z_send, z_recv, x_send, x_recv,
    own_sem, b_send, b_recv,
):
    S, E, ndoc, cap, RB, F, RP, nc, steps, pieces, tile = cfg
    s = lax.axis_index("seq")
    e = lax.axis_index("expert")
    q_rows, width = q_ref.shape
    shard = k_ref.shape[0]
    kvl = k_ref.shape[1] // HD
    group = width // HD // kvl
    T = routes_ref.shape[1]
    ff = w_hbm.shape[1]
    depth = w_hbm.shape[0]
    scale = 1.0 / HD**0.5
    rows = S * RB

    def at_s(d):
        return lax.rem(s + S - d, S)

    def at_e(d):
        return lax.rem(e + E - d, E)

    barrier = pltpu.get_barrier_semaphore()
    for ds in range(S):
        for de in range(E):
            if ds or de:
                pl.semaphore_signal(
                    barrier, inc=1, device_id={"seq": at_s(ds), "expert": at_e(de)},
                    device_id_type=MESH,
                )

    def w_copy(r):
        src = lax.rem(e + r, E)
        return pltpu.make_async_copy(
            w_hbm.at[pl.ds(pl.multiple_of(src * width, width), width)], wbuf.at[r], w_sem.at[r]
        )

    for r in range(E):
        w_copy(r).start()
    pl.semaphore_wait(barrier, S * E - 1)

    def remote(src, dst, ssem, rsem, ds, de):
        return pltpu.make_async_remote_copy(
            src_ref=src, dst_ref=dst, send_sem=ssem, recv_sem=rsem,
            device_id={"seq": at_s(ds), "expert": at_e(de)}, device_id_type=MESH,
        )

    kv_copies = []
    offset = 0
    for i, (d, first) in enumerate(pieces):
        n = shard - first
        kc = remote(k_ref.at[pl.ds(first, n)], kbuf.at[pl.ds(offset, n)],
                    kv_send.at[2 * i], kv_recv.at[2 * i], S - d, 0)
        vc = remote(v_ref.at[pl.ds(first, n)], vbuf.at[pl.ds(offset, n)],
                    kv_send.at[2 * i + 1], kv_recv.at[2 * i + 1], S - d, 0)
        kc.start()
        vc.start()
        kv_copies += [kc, vc]
        offset += n
    r_copies = []
    for de in range(1, E):
        c = remote(routes_ref, rbuf.at[de], r_send.at[de], r_recv.at[de], 0, de)
        c.start()
        r_copies.append(c)

    qn = group * q_rows
    qpos = s * shard + shard - q_rows + lax.rem(iota((qn, 1), 0), q_rows)
    docstart = jnp.zeros((qn, 1), jnp.int32)
    begin = jnp.int32(0)
    for j in range(ndoc):
        docstart = jnp.where(qpos >= begin, begin, docstart)
        begin = begin + len_ref[j]

    def masked(q, k, first):
        sc = lax.dot_general(q, k, NT, preferred_element_type=F32) * scale
        kpos = first + iota((1, k.shape[0]), 1)
        return jnp.where((kpos <= qpos) & (kpos >= docstart), sc, F32(-1e30))

    queries = []
    local = []
    for h in range(kvl):
        q = jnp.concatenate(
            [q_ref[:, (h * group + g) * HD:(h * group + g + 1) * HD] for g in range(group)], axis=0
        )
        queries.append(q)
        local.append(masked(q, k_ref[:, h * HD:(h + 1) * HD], s * shard))

    for c in r_copies:
        c.wait()
    mine = routes_ref[...]
    names = iota((up(E, 8), 1), 0)

    def members(rt):
        return onehot((rt[0:1, :] == names) | (rt[1:2, :] == names))

    upper = onehot(iota((T, T), 0) < iota((T, T), 1))
    blocks = []
    for de in range(E):
        mt = members(mine if de == 0 else rbuf[de])
        cnt = dot(mt, upper)
        blk = lax.rem(e + de, E)
        place = jnp.where(mt > 0.5, cnt + (blk * cap).astype(F32), F32(-1.0))
        blocks.append((place, blk))
        if de == 0:
            before = cnt
    Q = q_rows
    total_place = jnp.zeros((up(E, 8), Q), F32)
    for place, blk in blocks:
        shift = onehot(iota((T, Q), 0) + blk * T == iota((T, Q), 1))
        total_place = total_place + dot((place + 1.0).astype(BF16), shift)
    row_of = iota((RB, Q), 0).astype(F32) + 1.0
    sel = []
    for x in range(E):
        sel.append(onehot(total_place[x:x + 1, :] == row_of))
    selector = jnp.concatenate(sel, axis=0)

    for c in kv_copies:
        c.wait()
    for h in range(kvl):
        q = queries[h]
        hs = slice(h * HD, (h + 1) * HD)
        parts = [(local[h], v_ref[:, hs])]
        offset = 0
        for d, first in pieces:
            n = shard - first
            parts.append((masked(q, kbuf[offset:offset + n, hs], (s - d) * shard + first),
                          vbuf[offset:offset + n, hs]))
            offset += n
        peak = jnp.max(parts[0][0], axis=-1, keepdims=True)
        for sc, _ in parts[1:]:
            peak = jnp.maximum(peak, jnp.max(sc, axis=-1, keepdims=True))
        total, got = None, None
        for sc, v in parts:
            wt = jnp.exp(sc - peak)
            t = jnp.sum(wt, axis=-1, keepdims=True)
            o = dot(wt.astype(BF16), v)
            total = t if total is None else total + t
            got = o if got is None else got + o
        att = (got / total).astype(BF16)
        for g in range(group):
            cols = slice((h * group + g) * HD, (h * group + g + 1) * HD)
            packed = dot(selector, att[g * q_rows:(g + 1) * q_rows]).astype(BF16)
            for x in range(E):
                pack[x, :, cols] = packed[x * RB:(x + 1) * RB]

    mine_rows = pl.ds(pl.multiple_of(s * RB, RB), RB)

    z_copies = [None]
    for r in range(1, E):
        c = remote(pack.at[at_e(r)], xbuf.at[r, mine_rows], z_send.at[r], z_recv.at[r], 0, r)
        c.start()
        z_copies.append(c)
    x_copies = []
    for ds in range(1, S):
        c = remote(pack.at[e], xbuf.at[0, mine_rows], x_send.at[0, ds], x_recv.at[0, ds], ds, 0)
        c.start()
        x_copies.append(c)
    own = pltpu.make_async_copy(pack.at[e], xbuf.at[0, mine_rows], own_sem.at[0])
    own.start()

    rows_out, rows_in = E * S * RP, F * rows
    out_row = iota((rows_out, 1), 0)
    inner = lax.rem(out_row, RP)
    which = lax.div(out_row, RP)
    ds_of = lax.rem(which, S)
    de_of = lax.div(which, S)
    f_of = lax.div(inner, cap)
    slot_of = lax.rem(inner, cap)
    s_of = lax.rem(s + S - ds_of, S)
    e_of = lax.rem(e + E - de_of, E)
    from_row = f_of * rows + s_of * RB + e_of * cap + slot_of
    from_row = jnp.where(inner < F * cap, from_row, -1)
    perm = onehot(from_row == iota((rows_out, rows_in), 1))

    diagonal = iota((T, T), 0) == iota((T, T), 1)

    def column(row):
        return jnp.sum(jnp.where(diagonal, row, jnp.zeros_like(row)), axis=1, keepdims=True)

    picks = []
    wide = iota((T, E * RP), 1)
    at = []
    for k in range(2):
        rk = mine[k:k + 1, :]
        slot = jnp.sum(jnp.where(rk == names, before, F32(0.0)), axis=0, keepdims=True)
        rel = rk - e
        rel = jnp.where(rel < 0, rel + E, rel)
        at.append(column((rel * RP).astype(F32) + slot).astype(jnp.int32))
    for f in range(F):
        for k in range(2):
            picks.append(onehot(at[k] + f * cap == wide))
    pick = jnp.concatenate(picks, axis=0)

    square = jnp.zeros((rows, 1), F32)
    sends = []
    for r in range(E):
        if r + 1 < E:
            z_copies[r + 1].wait()
            for ds in range(1, S):
                c = remote(xbuf.at[r + 1, mine_rows], xbuf.at[r + 1, mine_rows],
                           x_send.at[r + 1, ds], x_recv.at[r + 1, ds], ds, 0)
                c.start()
                x_copies.append(c)
        if r == 0:
            own.wait()
        for c in x_copies[r * (S - 1):(r + 1) * (S - 1)]:
            c.wait()
        w_copy(r).wait()
        x = xbuf[r]
        xf = x.astype(F32)
        square = square + jnp.sum(xf * xf, axis=-1, keepdims=True)
        if r < E - 1:
            def body(i, carry, r=r, x=x):
                cols = pl.ds(pl.multiple_of(i * tile, tile), tile)
                part = dot(x, wbuf[r, :, cols])
                if r == 0:
                    acc[:, cols] = part
                else:
                    acc[:, cols] += part
                return carry

            lax.fori_loop(0, ff // tile, body, 0)
        else:
            factor = lax.rsqrt(square / depth + 1e-05)
            for st, (c0, n) in enumerate(steps):
                folded = []
                for f in range(F):
                    cols = slice(f * nc + c0, f * nc + c0 + n)
                    part = dot(x, wbuf[r, :, cols])
                    if r > 0:
                        part = part + acc[:, cols]
                    part = part * factor
                    folded.append((part / (1.0 + jnp.exp(-part))).astype(BF16))
                moved = dot(perm, jnp.concatenate(folded, axis=0)).astype(BF16)
                for de in reversed(range(E)):
                    for ds in reversed(range(S)):
                        base = (de * S + ds) * RP
                        block = moved[base:base + RP]
                        if ds or de:
                            sendbuf[de, ds, :, c0:c0 + n] = block
                        else:
                            recv[0, 0, :, c0:c0 + n] = block
                for de in reversed(range(E)):
                    for ds in reversed(range(S)):
                        if ds or de:
                            c = remote(sendbuf.at[de, ds, :, pl.ds(c0, n)],
                                       recv.at[ds, de, :, pl.ds(c0, n)],
                                       b_send.at[st, de, ds], b_recv.at[st, de, ds], ds, de)
                            c.start()
                            sends.append((st, ds, c))

    g0, g1 = column(gates_ref[0:1, :]), column(gates_ref[1:2, :])
    for st, (c0, n) in enumerate(steps):
        for ds in range(S):
            for a, b, c in sends:
                if a == st and b == ds:
                    c.wait()
            got = recv[ds, :, :, c0:c0 + n].reshape(E * RP, n)
            res = dot(pick, got)
            base = lax.rem(s + ds, S) * ff
            for f in range(F):
                lo = 2 * f * T
                mix = g0 * res[lo:lo + T] + g1 * res[lo + T:lo + 2 * T]
                cols = pl.ds(pl.multiple_of(base + (f * nc + c0), 128), n)
                out_ref[:, cols] = mix.astype(BF16)


def shards(queries, keys, values, lengths, routes, gates, w_up):
    S, E = lax.axis_size("seq"), lax.axis_size("expert")
    q_rows, width = queries.shape
    shard = keys.shape[0]
    w = w_up.reshape(w_up.shape[1], w_up.shape[2])
    depth, ff = w.shape
    T = routes.shape[0]
    cap = max(2, 3 * q_rows // (E * E))
    RB = up(E * cap, 16)
    choices = [f for f in range(1, ff // 128 + 1) if ff % (f * 128) == 0]
    F = min(choices, key=lambda f: up(f * cap, 16) * (ff // f))
    RP = up(F * cap, 16)
    nc = ff // F
    half = up(nc // 2, 256)
    steps = [(0, nc)] if half >= nc else [(0, half), (half, nc - half)]
    tile = 512 if ff % 512 == 0 else 128
    window = shard * S // 2
    pieces = []
    for d in range(1, S):
        first = max(0, (d + 1) * shard - q_rows - window + 1) // 16 * 16
        if first < shard:
            pieces.append((d, first))
    kv_rows = sum(shard - first for _, first in pieces)
    cfg = (S, E, lengths.shape[0], cap, RB, F, RP, nc, steps, pieces, tile)
    vmem = pl.BlockSpec(memory_space=pltpu.VMEM)
    dma = pltpu.SemaphoreType.DMA
    return pl.pallas_call(
        functools.partial(kernel, cfg),
        out_shape=jax.ShapeDtypeStruct((T, S * ff), BF16),
        in_specs=[pl.BlockSpec(memory_space=pltpu.SMEM), vmem, vmem, vmem, vmem, vmem,
                  pl.BlockSpec(memory_space=pl.ANY)],
        out_specs=vmem,
        scratch_shapes=[
            pltpu.VMEM((E, width, ff), BF16),
            pltpu.VMEM((kv_rows, keys.shape[1]), BF16),
            pltpu.VMEM((kv_rows, keys.shape[1]), BF16),
            pltpu.VMEM((E, 2, T), jnp.int32),
            pltpu.VMEM((E, RB, width), BF16),
            pltpu.VMEM((E, S * RB, width), BF16),
            pltpu.VMEM((S * RB, ff), F32),
            pltpu.VMEM((E, S, RP, nc), BF16),
            pltpu.VMEM((S, E, RP, nc), BF16),
            dma((E,)),
            dma((2 * len(pieces),)),
            dma((2 * len(pieces),)),
            dma((E,)), dma((E,)), dma((E,)), dma((E,)),
            dma((E, S)), dma((E, S)),
            dma((1,)),
            dma((len(steps), E, S)), dma((len(steps), E, S)),
        ],
        compiler_params=pltpu.CompilerParams(
            collective_id=0, has_side_effects=True, vmem_limit_bytes=60 * 1024 * 1024
        ),
    )(lengths, queries, keys, values, routes.T, gates.T, w)


def solution(mesh):
    placed = (
        P(("dp", "seq"), "expert"),
        P(("dp", "seq"), "expert"),
        P(("dp", "seq"), "expert"),
        P("dp"),
        P(("dp", "seq", "expert"), None),
        P(("dp", "seq", "expert"), None),
        P("expert", None, "seq"),
    )
    return jax.shard_map(
        shards,
        mesh=mesh,
        in_specs=placed,
        out_specs=P(("dp", "seq", "expert"), None),
        check_vma=False,
    )
```

```python
import functools

import jax
import jax.numpy as jnp
from jax import lax
from jax.experimental import pallas as pl
from jax.experimental.pallas import tpu as pltpu
from jax.sharding import PartitionSpec as P

HD = 128
MESH = pl.DeviceIdType.MESH
F32 = jnp.float32
BF16 = jnp.bfloat16
NT = (((1,), (1,)), ((), ()))


def up(n, m):
    return -(-n // m) * m


def iota(shape, dim):
    return lax.broadcasted_iota(jnp.int32, shape, dim)


def onehot(mask):
    return jnp.where(mask, F32(1.0), F32(0.0)).astype(BF16)


def dot(a, b):
    return jnp.dot(a, b, preferred_element_type=F32)


def kernel(
    cfg,
    len_hbm, q_hbm, k_hbm, v_hbm, routes_hbm, gates_hbm, w_hbm, out_hbm,
    len_ref, q_ref, k_ref, v_ref, routes_ref, gates_ref, out_ref,
    wbuf, kbuf, vbuf, rbuf, pack, xbuf, acc, sendbuf, recv,
    in_sem, w_sem, kv_send, kv_recv, r_send, r_recv, z_send, z_recv, x_send, x_recv,
    own_sem, b_send, b_recv, out_sem,
):
    S, E, ndoc, cap, RB, F, RP, nc, steps, pieces, tile = cfg
    s = lax.axis_index("seq")
    e = lax.axis_index("expert")
    q_rows, width = q_ref.shape
    shard = k_ref.shape[0]
    kvl = k_ref.shape[1] // HD
    group = width // HD // kvl
    T = routes_ref.shape[1]
    ff = w_hbm.shape[1]
    depth = w_hbm.shape[0]
    scale = 1.0 / HD**0.5

    def at_s(d):
        return lax.rem(s + S - d, S)

    def at_e(d):
        return lax.rem(e + E - d, E)

    barrier = pltpu.get_barrier_semaphore()
    for ds in range(S):
        for de in range(E):
            if ds or de:
                pl.semaphore_signal(
                    barrier, inc=1, device_id={"seq": at_s(ds), "expert": at_e(de)},
                    device_id_type=MESH,
                )

    def w_copy(r):
        src = lax.rem(e + r, E)
        return pltpu.make_async_copy(
            w_hbm.at[pl.ds(pl.multiple_of(src * width, width), width)], wbuf.at[r], w_sem.at[r]
        )

    ins = []
    for i, (src, dst) in enumerate((
        (k_hbm, k_ref), (v_hbm, v_ref), (routes_hbm, routes_ref), (q_hbm, q_ref),
        (len_hbm, len_ref), (gates_hbm, gates_ref),
    )):
        c = pltpu.make_async_copy(src, dst, in_sem.at[i])
        c.start()
        ins.append(c)
    for r in range(E):
        w_copy(r).start()
    for c in ins[:3]:
        c.wait()
    pl.semaphore_wait(barrier, S * E - 1)

    def remote(src, dst, ssem, rsem, ds, de):
        return pltpu.make_async_remote_copy(
            src_ref=src, dst_ref=dst, send_sem=ssem, recv_sem=rsem,
            device_id={"seq": at_s(ds), "expert": at_e(de)}, device_id_type=MESH,
        )

    kv_copies = []
    offset = 0
    for i, (d, first) in enumerate(pieces):
        n = shard - first
        kc = remote(k_ref.at[pl.ds(first, n)], kbuf.at[pl.ds(offset, n)],
                    kv_send.at[2 * i], kv_recv.at[2 * i], S - d, 0)
        vc = remote(v_ref.at[pl.ds(first, n)], vbuf.at[pl.ds(offset, n)],
                    kv_send.at[2 * i + 1], kv_recv.at[2 * i + 1], S - d, 0)
        kc.start()
        vc.start()
        kv_copies += [kc, vc]
        offset += n
    r_copies = []
    for de in range(1, E):
        c = remote(routes_ref, rbuf.at[de], r_send.at[de], r_recv.at[de], 0, de)
        c.start()
        r_copies.append(c)

    for c in ins[3:]:
        c.wait()
    qn = group * q_rows
    qpos = s * shard + shard - q_rows + lax.rem(iota((qn, 1), 0), q_rows)
    docstart = jnp.zeros((qn, 1), jnp.int32)
    begin = jnp.int32(0)
    for j in range(ndoc):
        docstart = jnp.where(qpos >= begin, begin, docstart)
        begin = begin + len_ref[j]

    def masked(q, k, first):
        sc = lax.dot_general(q, k, NT, preferred_element_type=F32) * scale
        kpos = first + iota((1, k.shape[0]), 1)
        return jnp.where((kpos <= qpos) & (kpos >= docstart), sc, F32(-1e30))

    queries = []
    local = []
    for h in range(kvl):
        q = jnp.concatenate(
            [q_ref[:, (h * group + g) * HD:(h * group + g + 1) * HD] for g in range(group)], axis=0
        )
        queries.append(q)
        local.append(masked(q, k_ref[:, h * HD:(h + 1) * HD], s * shard))

    for c in r_copies:
        c.wait()
    mine = routes_ref[...]
    names = iota((up(E, 8), 1), 0)

    def members(rt):
        return onehot((rt[0:1, :] == names) | (rt[1:2, :] == names))

    upper = onehot(iota((T, T), 0) < iota((T, T), 1))
    blocks = []
    for de in range(E):
        mt = members(mine if de == 0 else rbuf[de])
        cnt = dot(mt, upper)
        blk = lax.rem(e + de, E)
        place = jnp.where(mt > 0.5, cnt + (blk * cap).astype(F32), F32(-1.0))
        blocks.append((place, blk))
        if de == 0:
            before = cnt
    Q = q_rows
    total_place = jnp.zeros((up(E, 8), Q), F32)
    for place, blk in blocks:
        shift = onehot(iota((T, Q), 0) + blk * T == iota((T, Q), 1))
        total_place = total_place + dot((place + 1.0).astype(BF16), shift)
    row_of = iota((RB, Q), 0).astype(F32) + 1.0
    sel = []
    for x in range(E):
        sel.append(onehot(total_place[x:x + 1, :] == row_of))
    selector = jnp.concatenate(sel, axis=0)

    for c in kv_copies:
        c.wait()
    hw = group * HD
    z_copies, x_copies, own_copies = {}, {}, []

    def relay(r, h, src):
        for ds in range(1, S):
            c = remote(src, xbuf.at[S - ds, r, :, pl.ds(h * hw, hw)],
                       x_send.at[h, r, ds], x_recv.at[h, r, S - ds], ds, 0)
            c.start()
            x_copies[h, r, ds] = c

    def send_head(h):
        part = pl.ds(h * hw, hw)
        for r in range(1, E):
            c = remote(pack.at[at_e(r), :, part], xbuf.at[0, r, :, part],
                       z_send.at[h, r], z_recv.at[h, r], 0, r)
            c.start()
            z_copies[h, r] = c
        relay(0, h, pack.at[e, :, part])
        own = pltpu.make_async_copy(pack.at[e, :, part], xbuf.at[0, 0, :, part], own_sem.at[h])
        own.start()
        own_copies.append(own)

    for h in range(kvl):
        q = queries[h]
        hs = slice(h * HD, (h + 1) * HD)
        parts = [(local[h], v_ref[:, hs])]
        offset = 0
        for d, first in pieces:
            n = shard - first
            parts.append((masked(q, kbuf[offset:offset + n, hs], (s - d) * shard + first),
                          vbuf[offset:offset + n, hs]))
            offset += n
        peak = jnp.max(parts[0][0], axis=-1, keepdims=True)
        for sc, _ in parts[1:]:
            peak = jnp.maximum(peak, jnp.max(sc, axis=-1, keepdims=True))
        total, got = None, None
        for sc, v in parts:
            wt = jnp.exp(sc - peak)
            t = jnp.sum(wt, axis=-1, keepdims=True)
            o = dot(wt.astype(BF16), v)
            total = t if total is None else total + t
            got = o if got is None else got + o
        att = (got / total).astype(BF16)
        for g in range(group):
            cols = slice((h * group + g) * HD, (h * group + g + 1) * HD)
            packed = dot(selector, att[g * q_rows:(g + 1) * q_rows]).astype(BF16)
            for x in range(E):
                pack[x, :, cols] = packed[x * RB:(x + 1) * RB]
        send_head(h)

    rows_out, rows_in = E * RP, F * RB
    out_row = iota((rows_out, 1), 0)
    inner = lax.rem(out_row, RP)
    e_of = lax.rem(e + E - lax.div(out_row, RP), E)
    from_row = lax.div(inner, cap) * RB + e_of * cap + lax.rem(inner, cap)
    from_row = jnp.where(inner < F * cap, from_row, -1)
    perm = onehot(from_row == iota((rows_out, rows_in), 1))

    diagonal = iota((T, T), 0) == iota((T, T), 1)

    def column(row):
        return jnp.sum(jnp.where(diagonal, row, jnp.zeros_like(row)), axis=1, keepdims=True)

    picks = []
    wide = iota((T, E * RP), 1)
    at = []
    for k in range(2):
        rk = mine[k:k + 1, :]
        slot = jnp.sum(jnp.where(rk == names, before, F32(0.0)), axis=0, keepdims=True)
        rel = rk - e
        rel = jnp.where(rel < 0, rel + E, rel)
        at.append(column((rel * RP).astype(F32) + slot).astype(jnp.int32))
    for f in range(F):
        for k in range(2):
            picks.append(onehot(at[k] + f * cap == wide))
    pick = jnp.concatenate(picks, axis=0)

    sends = {}

    def squares(g, r):
        xf = xbuf[g, r].astype(F32)
        return jnp.sum(xf * xf, axis=-1, keepdims=True)

    def give_back(g, square, product):
        factor = lax.rsqrt(square / depth + 1e-05)
        for st, (c0, n) in enumerate(steps):
            folded = []
            for f in range(F):
                part = product(slice(f * nc + c0, f * nc + c0 + n)) * factor
                folded.append((part / (1.0 + jnp.exp(-part))).astype(BF16))
            moved = dot(perm, jnp.concatenate(folded, axis=0)).astype(BF16)
            for de in range(E):
                block = moved[de * RP:(de + 1) * RP]
                if g or de:
                    sendbuf[de, g, :, c0:c0 + n] = block
                else:
                    recv[0, 0, :, c0:c0 + n] = block
            for de in reversed(range(E)):
                if g or de:
                    c = remote(sendbuf.at[de, g, :, pl.ds(c0, n)],
                               recv.at[g, de, :, pl.ds(c0, n)],
                               b_send.at[st, de, g], b_recv.at[st, de, g], g, de)
                    c.start()
                    sends[st, de, g] = c

    square = jnp.zeros((RB, 1), F32)
    for r in range(E):
        for h in range(kvl):
            if r:
                z_copies[h, r].wait()
                relay(r, h, xbuf.at[0, r, :, pl.ds(h * hw, hw)])
            else:
                own_copies[h].wait()
        w_copy(r).wait()
        square = square + squares(0, r)
        x = xbuf[0, r]
        if r < E - 1:
            def body(i, carry, r=r, x=x):
                cols = pl.ds(pl.multiple_of(i * tile, tile), tile)
                part = dot(x, wbuf[r, :, cols])
                if r == 0:
                    acc[:, cols] = part
                else:
                    acc[:, cols] += part
                return carry

            lax.fori_loop(0, ff // tile, body, 0)
        else:
            def last(cols, r=r, x=x):
                part = dot(x, wbuf[r, :, cols])
                return part + acc[:, cols] if r else part

            give_back(0, square, last)
    for g in range(1, S):
        square = jnp.zeros((RB, 1), F32)
        for r in range(E):
            for h in range(kvl):
                x_copies[h, r, S - g].wait_recv()
            square = square + squares(g, r)

        def whole(cols, g=g):
            part = dot(xbuf[g, 0], wbuf[0, :, cols])
            for r in range(1, E):
                part = part + dot(xbuf[g, r], wbuf[r, :, cols])
            return part

        give_back(g, square, whole)
    for c in x_copies.values():
        c.wait_send()

    g0, g1 = column(gates_ref[0:1, :]), column(gates_ref[1:2, :])
    outs = []
    for g in range(S):
        base = pl.multiple_of(lax.rem(s + g, S) * ff, 128)
        for st, (c0, n) in enumerate(steps):
            for de in range(E):
                if g or de:
                    sends[st, de, g].wait()
            got = recv[g, :, :, c0:c0 + n].reshape(E * RP, n)
            res = dot(pick, got)
            for f in range(F):
                lo = 2 * f * T
                mix = g0 * res[lo:lo + T] + g1 * res[lo + T:lo + 2 * T]
                cols = slice(f * nc + c0, f * nc + c0 + n)
                out_ref[g, :, cols] = mix.astype(BF16)
        c = pltpu.make_async_copy(out_ref.at[g], out_hbm.at[:, pl.ds(base, ff)], out_sem.at[g])
        c.start()
        outs.append(c)
    for c in outs:
        c.wait()


def shards(queries, keys, values, lengths, routes, gates, w_up):
    S, E = lax.axis_size("seq"), lax.axis_size("expert")
    q_rows, width = queries.shape
    shard = keys.shape[0]
    w = w_up.reshape(w_up.shape[1], w_up.shape[2])
    depth, ff = w.shape
    T = routes.shape[0]
    cap = max(2, 3 * q_rows // (E * E))
    RB = up(E * cap, 16)
    choices = [f for f in range(1, ff // 128 + 1) if ff % (f * 128) == 0]
    F = min(choices, key=lambda f: up(f * cap, 16) * (ff // f))
    RP = up(F * cap, 16)
    nc = ff // F
    cuts = list(range(0, max(nc - 255, 1), 256))
    steps = [(c, (cuts + [nc])[i + 1] - c) for i, c in enumerate(cuts)]
    tile = 512 if ff % 512 == 0 else 128
    window = shard * S // 2
    pieces = []
    for d in range(1, S):
        first = max(0, (d + 1) * shard - q_rows - window + 1) // 16 * 16
        if first < shard:
            pieces.append((d, first))
    kv_rows = sum(shard - first for _, first in pieces)
    cfg = (S, E, lengths.shape[0], cap, RB, F, RP, nc, steps, pieces, tile)
    kvl = keys.shape[1] // HD
    dma = pltpu.SemaphoreType.DMA
    return pl.pallas_call(
        functools.partial(kernel, cfg),
        out_shape=jax.ShapeDtypeStruct((T, S * ff), BF16),
        in_specs=[pl.BlockSpec(memory_space=pl.ANY)] * 7,
        out_specs=pl.BlockSpec(memory_space=pl.ANY),
        scratch_shapes=[
            pltpu.SMEM(lengths.shape, jnp.int32),
            pltpu.VMEM(queries.shape, BF16),
            pltpu.VMEM(keys.shape, BF16),
            pltpu.VMEM(values.shape, BF16),
            pltpu.VMEM((2, T), jnp.int32),
            pltpu.VMEM((2, T), F32),
            pltpu.VMEM((S, T, ff), BF16),
            pltpu.VMEM((E, width, ff), BF16),
            pltpu.VMEM((kv_rows, keys.shape[1]), BF16),
            pltpu.VMEM((kv_rows, keys.shape[1]), BF16),
            pltpu.VMEM((E, 2, T), jnp.int32),
            pltpu.VMEM((E, RB, width), BF16),
            pltpu.VMEM((S, E, RB, width), BF16),
            pltpu.VMEM((RB, ff), F32),
            pltpu.VMEM((E, S, RP, nc), BF16),
            pltpu.VMEM((S, E, RP, nc), BF16),
            dma((6,)),
            dma((E,)),
            dma((2 * len(pieces),)),
            dma((2 * len(pieces),)),
            dma((E,)), dma((E,)), dma((kvl, E)), dma((kvl, E)),
            dma((kvl, E, S)), dma((kvl, E, S)),
            dma((kvl,)),
            dma((len(steps), E, S)), dma((len(steps), E, S)),
            dma((S,)),
        ],
        compiler_params=pltpu.CompilerParams(
            collective_id=0, has_side_effects=True, vmem_limit_bytes=60 * 1024 * 1024
        ),
    )(lengths, queries, keys, values, routes.T, gates.T, w)


def solution(mesh):
    placed = (
        P(("dp", "seq"), "expert"),
        P(("dp", "seq"), "expert"),
        P(("dp", "seq"), "expert"),
        P("dp"),
        P(("dp", "seq", "expert"), None),
        P(("dp", "seq", "expert"), None),
        P("expert", None, "seq"),
    )
    return jax.shard_map(
        shards,
        mesh=mesh,
        in_specs=placed,
        out_specs=P(("dp", "seq", "expert"), None),
        check_vma=False,
    )
```

```python
import functools

import jax
import jax.numpy as jnp
from jax import lax
from jax.experimental import pallas as pl
from jax.experimental.pallas import tpu as pltpu
from jax.sharding import PartitionSpec as P

HD = 128
MESH = pl.DeviceIdType.MESH
F32 = jnp.float32
BF16 = jnp.bfloat16
NT = (((1,), (1,)), ((), ()))


def up(n, m):
    return -(-n // m) * m


def iota(shape, dim):
    return lax.broadcasted_iota(jnp.int32, shape, dim)


def onehot(mask):
    return jnp.where(mask, F32(1.0), F32(0.0)).astype(BF16)


def dot(a, b):
    return jnp.dot(a, b, preferred_element_type=F32)


def kernel(
    cfg,
    len_hbm, q_hbm, k_hbm, v_hbm, routes_hbm, gates_hbm, w_hbm, out_hbm,
    len_ref, q_ref, k_ref, v_ref, routes_ref, gates_ref, out_ref,
    wbuf, kbuf, vbuf, rbuf, pack, xbuf, acc, sendbuf, recv,
    in_sem, w_sem, kv_send, kv_recv, r_send, r_recv, z_send, z_recv, x_send, x_recv,
    own_sem, b_send, b_recv, out_sem,
):
    S, E, ndoc, cap, RB, F, RP, nc, steps, pieces, tile = cfg
    s = lax.axis_index("seq")
    e = lax.axis_index("expert")
    q_rows, width = q_ref.shape
    shard = k_ref.shape[0]
    kvl = k_ref.shape[1] // HD
    group = width // HD // kvl
    T = routes_ref.shape[1]
    ff = w_hbm.shape[1]
    depth = w_hbm.shape[0]
    scale = 1.0 / HD**0.5

    def at_s(d):
        return lax.rem(s + S - d, S)

    def at_e(d):
        return lax.rem(e + E - d, E)

    barrier = pltpu.get_barrier_semaphore()
    for ds in range(S):
        for de in range(E):
            if ds or de:
                pl.semaphore_signal(
                    barrier, inc=1, device_id={"seq": at_s(ds), "expert": at_e(de)},
                    device_id_type=MESH,
                )

    def w_copy(r):
        src = lax.rem(e + r, E)
        return pltpu.make_async_copy(
            w_hbm.at[pl.ds(pl.multiple_of(src * width, width), width)], wbuf.at[r], w_sem.at[r]
        )

    ins = []
    for i, (src, dst) in enumerate((
        (k_hbm, k_ref), (v_hbm, v_ref), (routes_hbm, routes_ref), (q_hbm, q_ref),
        (len_hbm, len_ref), (gates_hbm, gates_ref),
    )):
        c = pltpu.make_async_copy(src, dst, in_sem.at[i])
        c.start()
        ins.append(c)
    for r in range(E):
        w_copy(r).start()
    for c in ins[:3]:
        c.wait()
    pl.semaphore_wait(barrier, S * E - 1)

    def remote(src, dst, ssem, rsem, ds, de):
        return pltpu.make_async_remote_copy(
            src_ref=src, dst_ref=dst, send_sem=ssem, recv_sem=rsem,
            device_id={"seq": at_s(ds), "expert": at_e(de)}, device_id_type=MESH,
        )

    kv_copies = []
    offset = 0
    for i, (d, first) in enumerate(pieces):
        n = shard - first
        kc = remote(k_ref.at[pl.ds(first, n)], kbuf.at[pl.ds(offset, n)],
                    kv_send.at[2 * i], kv_recv.at[2 * i], S - d, 0)
        vc = remote(v_ref.at[pl.ds(first, n)], vbuf.at[pl.ds(offset, n)],
                    kv_send.at[2 * i + 1], kv_recv.at[2 * i + 1], S - d, 0)
        kc.start()
        vc.start()
        kv_copies += [kc, vc]
        offset += n
    r_copies = []
    for de in range(1, E):
        c = remote(routes_ref, rbuf.at[de], r_send.at[de], r_recv.at[de], 0, de)
        c.start()
        r_copies.append(c)

    for c in ins[3:]:
        c.wait()
    qn = group * q_rows
    qpos = s * shard + shard - q_rows + lax.rem(iota((qn, 1), 0), q_rows)
    docstart = jnp.zeros((qn, 1), jnp.int32)
    begin = jnp.int32(0)
    for j in range(ndoc):
        docstart = jnp.where(qpos >= begin, begin, docstart)
        begin = begin + len_ref[j]

    def masked(q, k, first):
        sc = lax.dot_general(q, k, NT, preferred_element_type=F32) * scale
        kpos = first + iota((1, k.shape[0]), 1)
        return jnp.where((kpos <= qpos) & (kpos >= docstart), sc, F32(-1e30))

    queries = []
    local = []
    for h in range(kvl):
        q = jnp.concatenate(
            [q_ref[:, (h * group + g) * HD:(h * group + g + 1) * HD] for g in range(group)], axis=0
        )
        queries.append(q)
        sc = masked(q, k_ref[:, h * HD:(h + 1) * HD], s * shard)
        peak = jnp.max(sc, axis=-1, keepdims=True)
        wt = jnp.exp(sc - peak)
        local.append((peak, jnp.sum(wt, axis=-1, keepdims=True),
                      dot(wt.astype(BF16), v_ref[:, h * HD:(h + 1) * HD])))

    for c in r_copies:
        c.wait()
    mine = routes_ref[...]
    names = iota((up(E, 8), 1), 0)

    def members(rt):
        return onehot((rt[0:1, :] == names) | (rt[1:2, :] == names))

    upper = onehot(iota((T, T), 0) < iota((T, T), 1))
    blocks = []
    for de in range(E):
        mt = members(mine if de == 0 else rbuf[de])
        cnt = dot(mt, upper)
        blk = lax.rem(e + de, E)
        place = jnp.where(mt > 0.5, cnt + (blk * cap).astype(F32), F32(-1.0))
        blocks.append((place, blk))
        if de == 0:
            before = cnt
    Q = q_rows
    total_place = jnp.zeros((up(E, 8), Q), F32)
    for place, blk in blocks:
        shift = onehot(iota((T, Q), 0) + blk * T == iota((T, Q), 1))
        total_place = total_place + dot((place + 1.0).astype(BF16), shift)
    row_of = iota((RB, Q), 0).astype(F32) + 1.0
    sel = []
    for x in range(E):
        sel.append(onehot(total_place[x:x + 1, :] == row_of))
    selector = jnp.concatenate(sel, axis=0)

    for c in kv_copies:
        c.wait()
    hw = group * HD
    z_copies, x_copies, own_copies = {}, {}, []

    def relay(r, h, src):
        for ds in range(1, S):
            c = remote(src, xbuf.at[S - ds, r, :, pl.ds(h * hw, hw)],
                       x_send.at[h, r, ds], x_recv.at[h, r, S - ds], ds, 0)
            c.start()
            x_copies[h, r, ds] = c

    def send_head(h):
        part = pl.ds(h * hw, hw)
        for r in range(1, E):
            c = remote(pack.at[at_e(r), :, part], xbuf.at[0, r, :, part],
                       z_send.at[h, r], z_recv.at[h, r], 0, r)
            c.start()
            z_copies[h, r] = c
        relay(0, h, pack.at[e, :, part])
        own = pltpu.make_async_copy(pack.at[e, :, part], xbuf.at[0, 0, :, part], own_sem.at[h])
        own.start()
        own_copies.append(own)

    for h in range(kvl):
        q = queries[h]
        hs = slice(h * HD, (h + 1) * HD)
        peak, total, got = local[h]
        offset = 0
        for d, first in pieces:
            n = shard - first
            sc = masked(q, kbuf[offset:offset + n, hs], (s - d) * shard + first)
            higher = jnp.maximum(peak, jnp.max(sc, axis=-1, keepdims=True))
            wt = jnp.exp(sc - higher)
            fade = jnp.exp(peak - higher)
            total = total * fade + jnp.sum(wt, axis=-1, keepdims=True)
            got = got * fade + dot(wt.astype(BF16), vbuf[offset:offset + n, hs])
            peak = higher
            offset += n
        att = (got / total).astype(BF16)
        for g in range(group):
            cols = slice((h * group + g) * HD, (h * group + g + 1) * HD)
            packed = dot(selector, att[g * q_rows:(g + 1) * q_rows]).astype(BF16)
            for x in range(E):
                pack[x, :, cols] = packed[x * RB:(x + 1) * RB]
        send_head(h)

    rows_out, rows_in = E * RP, F * RB
    out_row = iota((rows_out, 1), 0)
    inner = lax.rem(out_row, RP)
    e_of = lax.rem(e + E - lax.div(out_row, RP), E)
    from_row = lax.div(inner, cap) * RB + e_of * cap + lax.rem(inner, cap)
    from_row = jnp.where(inner < F * cap, from_row, -1)
    perm = onehot(from_row == iota((rows_out, rows_in), 1))

    diagonal = iota((T, T), 0) == iota((T, T), 1)

    def column(row):
        return jnp.sum(jnp.where(diagonal, row, jnp.zeros_like(row)), axis=1, keepdims=True)

    picks = []
    wide = iota((T, E * RP), 1)
    at = []
    for k in range(2):
        rk = mine[k:k + 1, :]
        slot = jnp.sum(jnp.where(rk == names, before, F32(0.0)), axis=0, keepdims=True)
        rel = rk - e
        rel = jnp.where(rel < 0, rel + E, rel)
        at.append(column((rel * RP).astype(F32) + slot).astype(jnp.int32))
    for f in range(F):
        for k in range(2):
            picks.append(onehot(at[k] + f * cap == wide))
    pick = jnp.concatenate(picks, axis=0)

    sends = {}

    def squares(g, r):
        xf = xbuf[g, r].astype(F32)
        return jnp.sum(xf * xf, axis=-1, keepdims=True)

    def give_back(g, square, product):
        factor = lax.rsqrt(square / depth + 1e-05)
        for st, (c0, n) in enumerate(steps):
            folded = []
            for f in range(F):
                part = product(slice(f * nc + c0, f * nc + c0 + n)) * factor
                folded.append((part / (1.0 + jnp.exp(-part))).astype(BF16))
            moved = dot(perm, jnp.concatenate(folded, axis=0)).astype(BF16)
            for de in range(E):
                block = moved[de * RP:(de + 1) * RP]
                if g or de:
                    sendbuf[de, g, :, c0:c0 + n] = block
                else:
                    recv[0, 0, :, c0:c0 + n] = block
            for de in reversed(range(E)):
                if g or de:
                    c = remote(sendbuf.at[de, g, :, pl.ds(c0, n)],
                               recv.at[g, de, :, pl.ds(c0, n)],
                               b_send.at[st, de, g], b_recv.at[st, de, g], g, de)
                    c.start()
                    sends[st, de, g] = c

    square = jnp.zeros((RB, 1), F32)
    for r in range(E):
        for h in range(kvl):
            if r:
                z_copies[h, r].wait()
                relay(r, h, xbuf.at[0, r, :, pl.ds(h * hw, hw)])
            else:
                own_copies[h].wait()
        w_copy(r).wait()
        square = square + squares(0, r)
        x = xbuf[0, r]
        if r < E - 1:
            def body(i, carry, r=r, x=x):
                cols = pl.ds(pl.multiple_of(i * tile, tile), tile)
                part = dot(x, wbuf[r, :, cols])
                if r == 0:
                    acc[:, cols] = part
                else:
                    acc[:, cols] += part
                return carry

            lax.fori_loop(0, ff // tile, body, 0)
        else:
            def last(cols, r=r, x=x):
                part = dot(x, wbuf[r, :, cols])
                return part + acc[:, cols] if r else part

            give_back(0, square, last)
    for g in range(1, S):
        square = jnp.zeros((RB, 1), F32)
        for r in range(E):
            for h in range(kvl):
                x_copies[h, r, S - g].wait_recv()
            square = square + squares(g, r)

        def whole(cols, g=g):
            part = dot(xbuf[g, 0], wbuf[0, :, cols])
            for r in range(1, E):
                part = part + dot(xbuf[g, r], wbuf[r, :, cols])
            return part

        give_back(g, square, whole)
    for c in x_copies.values():
        c.wait_send()

    g0, g1 = column(gates_ref[0:1, :]), column(gates_ref[1:2, :])
    outs = []
    for g in range(S):
        base = pl.multiple_of(lax.rem(s + g, S) * ff, 128)
        for st, (c0, n) in enumerate(steps):
            for de in range(E):
                if g or de:
                    sends[st, de, g].wait()
            got = recv[g, :, :, c0:c0 + n].reshape(E * RP, n)
            res = dot(pick, got)
            for f in range(F):
                lo = 2 * f * T
                mix = g0 * res[lo:lo + T] + g1 * res[lo + T:lo + 2 * T]
                cols = slice(f * nc + c0, f * nc + c0 + n)
                out_ref[g, :, cols] = mix.astype(BF16)
        c = pltpu.make_async_copy(out_ref.at[g], out_hbm.at[:, pl.ds(base, ff)], out_sem.at[g])
        c.start()
        outs.append(c)
    for c in outs:
        c.wait()


def shards(queries, keys, values, lengths, routes, gates, w_up):
    S, E = lax.axis_size("seq"), lax.axis_size("expert")
    q_rows, width = queries.shape
    shard = keys.shape[0]
    w = w_up.reshape(w_up.shape[1], w_up.shape[2])
    depth, ff = w.shape
    T = routes.shape[0]
    cap = max(2, 3 * q_rows // (E * E))
    RB = up(E * cap, 16)
    choices = [f for f in range(1, ff // 128 + 1) if ff % (f * 128) == 0]
    F = min(choices, key=lambda f: up(f * cap, 16) * (ff // f))
    RP = up(F * cap, 16)
    nc = ff // F
    cuts = list(range(0, max(nc - 255, 1), 256))
    steps = [(c, (cuts + [nc])[i + 1] - c) for i, c in enumerate(cuts)]
    tile = 512 if ff % 512 == 0 else 128
    window = shard * S // 2
    pieces = []
    for d in range(1, S):
        first = max(0, (d + 1) * shard - q_rows - window + 1) // 16 * 16
        if first < shard:
            pieces.append((d, first))
    kv_rows = sum(shard - first for _, first in pieces)
    cfg = (S, E, lengths.shape[0], cap, RB, F, RP, nc, steps, pieces, tile)
    kvl = keys.shape[1] // HD
    dma = pltpu.SemaphoreType.DMA
    return pl.pallas_call(
        functools.partial(kernel, cfg),
        out_shape=jax.ShapeDtypeStruct((T, S * ff), BF16),
        in_specs=[pl.BlockSpec(memory_space=pl.ANY)] * 7,
        out_specs=pl.BlockSpec(memory_space=pl.ANY),
        scratch_shapes=[
            pltpu.SMEM(lengths.shape, jnp.int32),
            pltpu.VMEM(queries.shape, BF16),
            pltpu.VMEM(keys.shape, BF16),
            pltpu.VMEM(values.shape, BF16),
            pltpu.VMEM((2, T), jnp.int32),
            pltpu.VMEM((2, T), F32),
            pltpu.VMEM((S, T, ff), BF16),
            pltpu.VMEM((E, width, ff), BF16),
            pltpu.VMEM((kv_rows, keys.shape[1]), BF16),
            pltpu.VMEM((kv_rows, keys.shape[1]), BF16),
            pltpu.VMEM((E, 2, T), jnp.int32),
            pltpu.VMEM((E, RB, width), BF16),
            pltpu.VMEM((S, E, RB, width), BF16),
            pltpu.VMEM((RB, ff), F32),
            pltpu.VMEM((E, S, RP, nc), BF16),
            pltpu.VMEM((S, E, RP, nc), BF16),
            dma((6,)),
            dma((E,)),
            dma((2 * len(pieces),)),
            dma((2 * len(pieces),)),
            dma((E,)), dma((E,)), dma((kvl, E)), dma((kvl, E)),
            dma((kvl, E, S)), dma((kvl, E, S)),
            dma((kvl,)),
            dma((len(steps), E, S)), dma((len(steps), E, S)),
            dma((S,)),
        ],
        compiler_params=pltpu.CompilerParams(
            collective_id=0, has_side_effects=True, vmem_limit_bytes=60 * 1024 * 1024
        ),
    )(lengths, queries, keys, values, routes.T, gates.T, w)


def solution(mesh):
    placed = (
        P(("dp", "seq"), "expert"),
        P(("dp", "seq"), "expert"),
        P(("dp", "seq"), "expert"),
        P("dp"),
        P(("dp", "seq", "expert"), None),
        P(("dp", "seq", "expert"), None),
        P("expert", None, "seq"),
    )
    return jax.shard_map(
        shards,
        mesh=mesh,
        in_specs=placed,
        out_specs=P(("dp", "seq", "expert"), None),
        check_vma=False,
    )
```

```python
import functools

import jax
import jax.numpy as jnp
from jax import lax
from jax.experimental import pallas as pl
from jax.experimental.pallas import tpu as pltpu
from jax.sharding import PartitionSpec as P

HD = 128
MESH = pl.DeviceIdType.MESH
F32 = jnp.float32
BF16 = jnp.bfloat16
NT = (((1,), (1,)), ((), ()))


def up(n, m):
    return -(-n // m) * m


def iota(shape, dim):
    return lax.broadcasted_iota(jnp.int32, shape, dim)


def onehot(mask):
    return jnp.where(mask, F32(1.0), F32(0.0)).astype(BF16)


def dot(a, b):
    return jnp.dot(a, b, preferred_element_type=F32)


def kernel(
    cfg,
    len_hbm, q_hbm, k_hbm, v_hbm, routes_hbm, gates_hbm, w_hbm, out_hbm,
    len_ref, q_ref, k_ref, v_ref, routes_ref, gates_ref, out_ref,
    wbuf, kbuf, vbuf, rbuf, pack, xbuf, acc, sendbuf, recv,
    in_sem, w_sem, kv_send, kv_recv, r_send, r_recv, z_send, z_recv, x_send, x_recv,
    own_sem, b_send, b_recv, out_sem,
):
    S, E, ndoc, cap, RB, F, RP, nc, steps, pieces, tile = cfg
    s = lax.axis_index("seq")
    e = lax.axis_index("expert")
    q_rows, width = q_ref.shape
    shard = k_ref.shape[0]
    kvl = k_ref.shape[1] // HD
    group = width // HD // kvl
    T = routes_ref.shape[1]
    ff = w_hbm.shape[1]
    depth = w_hbm.shape[0]
    scale = 1.0 / HD**0.5

    def at_s(d):
        return lax.rem(s + S - d, S)

    def at_e(d):
        return lax.rem(e + E - d, E)

    barrier = pltpu.get_barrier_semaphore()
    for ds in range(S):
        for de in range(E):
            if ds or de:
                pl.semaphore_signal(
                    barrier, inc=1, device_id={"seq": at_s(ds), "expert": at_e(de)},
                    device_id_type=MESH,
                )

    def w_copy(r):
        src = lax.rem(e + r, E)
        return pltpu.make_async_copy(
            w_hbm.at[pl.ds(pl.multiple_of(src * width, width), width)], wbuf.at[r], w_sem.at[r]
        )

    ins = []
    for i, (src, dst) in enumerate((
        (k_hbm, k_ref), (v_hbm, v_ref), (routes_hbm, routes_ref), (q_hbm, q_ref),
        (len_hbm, len_ref), (gates_hbm, gates_ref),
    )):
        c = pltpu.make_async_copy(src, dst, in_sem.at[i])
        c.start()
        ins.append(c)
    for c in ins[:3]:
        c.wait()
    pl.semaphore_wait(barrier, S * E - 1)

    def remote(src, dst, ssem, rsem, ds, de):
        return pltpu.make_async_remote_copy(
            src_ref=src, dst_ref=dst, send_sem=ssem, recv_sem=rsem,
            device_id={"seq": at_s(ds), "expert": at_e(de)}, device_id_type=MESH,
        )

    kv_copies = []
    offset = 0
    for i, (d, first) in enumerate(pieces):
        n = shard - first
        kc = remote(k_ref.at[pl.ds(first, n)], kbuf.at[pl.ds(offset, n)],
                    kv_send.at[2 * i], kv_recv.at[2 * i], S - d, 0)
        vc = remote(v_ref.at[pl.ds(first, n)], vbuf.at[pl.ds(offset, n)],
                    kv_send.at[2 * i + 1], kv_recv.at[2 * i + 1], S - d, 0)
        kc.start()
        vc.start()
        kv_copies += [kc, vc]
        offset += n
    r_copies = []
    for de in range(1, E):
        c = remote(routes_ref, rbuf.at[de], r_send.at[de], r_recv.at[de], 0, de)
        c.start()
        r_copies.append(c)

    for c in ins[3:]:
        c.wait()
    for r in range(E):
        w_copy(r).start()
    qn = group * q_rows
    qpos = s * shard + shard - q_rows + lax.rem(iota((qn, 1), 0), q_rows)
    docstart = jnp.zeros((qn, 1), jnp.int32)
    begin = jnp.int32(0)
    for j in range(ndoc):
        docstart = jnp.where(qpos >= begin, begin, docstart)
        begin = begin + len_ref[j]

    def masked(q, k, first):
        sc = lax.dot_general(q, k, NT, preferred_element_type=F32) * scale
        kpos = first + iota((1, k.shape[0]), 1)
        return jnp.where((kpos <= qpos) & (kpos >= docstart), sc, F32(-1e30))

    queries = []
    local = []
    for h in range(kvl):
        q = jnp.concatenate(
            [q_ref[:, (h * group + g) * HD:(h * group + g + 1) * HD] for g in range(group)], axis=0
        )
        queries.append(q)
        sc = masked(q, k_ref[:, h * HD:(h + 1) * HD], s * shard)
        peak = jnp.max(sc, axis=-1, keepdims=True)
        wt = jnp.exp(sc - peak)
        local.append((peak, jnp.sum(wt, axis=-1, keepdims=True),
                      dot(wt.astype(BF16), v_ref[:, h * HD:(h + 1) * HD])))

    for c in r_copies:
        c.wait()
    mine = routes_ref[...]
    names = iota((up(E, 8), 1), 0)

    def members(rt):
        return onehot((rt[0:1, :] == names) | (rt[1:2, :] == names))

    upper = onehot(iota((T, T), 0) < iota((T, T), 1))
    blocks = []
    for de in range(E):
        mt = members(mine if de == 0 else rbuf[de])
        cnt = dot(mt, upper)
        blk = lax.rem(e + de, E)
        place = jnp.where(mt > 0.5, cnt + (blk * cap).astype(F32), F32(-1.0))
        blocks.append((place, blk))
        if de == 0:
            before = cnt
    Q = q_rows
    total_place = jnp.zeros((up(E, 8), Q), F32)
    for place, blk in blocks:
        shift = onehot(iota((T, Q), 0) + blk * T == iota((T, Q), 1))
        total_place = total_place + dot((place + 1.0).astype(BF16), shift)
    row_of = iota((RB, Q), 0).astype(F32) + 1.0
    sel = []
    for x in range(E):
        sel.append(onehot(total_place[x:x + 1, :] == row_of))
    selector = jnp.concatenate(sel, axis=0)

    for c in kv_copies:
        c.wait()
    hw = group * HD
    z_copies, x_copies, own_copies = {}, {}, []

    def relay(r, h, src):
        for ds in range(1, S):
            c = remote(src, xbuf.at[S - ds, r, :, pl.ds(h * hw, hw)],
                       x_send.at[h, r, ds], x_recv.at[h, r, S - ds], ds, 0)
            c.start()
            x_copies[h, r, ds] = c

    def send_head(h):
        part = pl.ds(h * hw, hw)
        for r in range(1, E):
            c = remote(pack.at[at_e(r), :, part], xbuf.at[0, r, :, part],
                       z_send.at[h, r], z_recv.at[h, r], 0, r)
            c.start()
            z_copies[h, r] = c
        relay(0, h, pack.at[e, :, part])
        own = pltpu.make_async_copy(pack.at[e, :, part], xbuf.at[0, 0, :, part], own_sem.at[h])
        own.start()
        own_copies.append(own)

    for h in range(kvl):
        q = queries[h]
        hs = slice(h * HD, (h + 1) * HD)
        peak, total, got = local[h]
        offset = 0
        for d, first in pieces:
            n = shard - first
            sc = masked(q, kbuf[offset:offset + n, hs], (s - d) * shard + first)
            higher = jnp.maximum(peak, jnp.max(sc, axis=-1, keepdims=True))
            wt = jnp.exp(sc - higher)
            fade = jnp.exp(peak - higher)
            total = total * fade + jnp.sum(wt, axis=-1, keepdims=True)
            got = got * fade + dot(wt.astype(BF16), vbuf[offset:offset + n, hs])
            peak = higher
            offset += n
        att = (got / total).astype(BF16)
        for g in range(group):
            cols = slice((h * group + g) * HD, (h * group + g + 1) * HD)
            packed = dot(selector, att[g * q_rows:(g + 1) * q_rows]).astype(BF16)
            for x in range(E):
                pack[x, :, cols] = packed[x * RB:(x + 1) * RB]
        send_head(h)

    rows_out, rows_in = E * RP, F * RB
    out_row = iota((rows_out, 1), 0)
    inner = lax.rem(out_row, RP)
    e_of = lax.rem(e + E - lax.div(out_row, RP), E)
    from_row = lax.div(inner, cap) * RB + e_of * cap + lax.rem(inner, cap)
    from_row = jnp.where(inner < F * cap, from_row, -1)
    perm = onehot(from_row == iota((rows_out, rows_in), 1))

    diagonal = iota((T, T), 0) == iota((T, T), 1)

    def column(row):
        return jnp.sum(jnp.where(diagonal, row, jnp.zeros_like(row)), axis=1, keepdims=True)

    picks = []
    wide = iota((T, E * RP), 1)
    at = []
    for k in range(2):
        rk = mine[k:k + 1, :]
        slot = jnp.sum(jnp.where(rk == names, before, F32(0.0)), axis=0, keepdims=True)
        rel = rk - e
        rel = jnp.where(rel < 0, rel + E, rel)
        at.append(column((rel * RP).astype(F32) + slot).astype(jnp.int32))
    for f in range(F):
        for k in range(2):
            picks.append(onehot(at[k] + f * cap == wide))
    pick = jnp.concatenate(picks, axis=0)

    sends = {}

    def squares(g, r):
        xf = xbuf[g, r].astype(F32)
        return jnp.sum(xf * xf, axis=-1, keepdims=True)

    def give_back(g, square, product):
        factor = lax.rsqrt(square / depth + 1e-05)
        for st, (c0, n) in enumerate(steps):
            folded = []
            for f in range(F):
                part = product(slice(f * nc + c0, f * nc + c0 + n)) * factor
                folded.append((part / (1.0 + jnp.exp(-part))).astype(BF16))
            moved = dot(perm, jnp.concatenate(folded, axis=0)).astype(BF16)
            for de in range(E):
                block = moved[de * RP:(de + 1) * RP]
                if g or de:
                    sendbuf[de, g, :, c0:c0 + n] = block
                else:
                    recv[0, 0, :, c0:c0 + n] = block
            for de in reversed(range(E)):
                if g or de:
                    c = remote(sendbuf.at[de, g, :, pl.ds(c0, n)],
                               recv.at[g, de, :, pl.ds(c0, n)],
                               b_send.at[st, de, g], b_recv.at[st, de, g], g, de)
                    c.start()
                    sends[st, de, g] = c

    square = jnp.zeros((RB, 1), F32)
    for r in range(E):
        for h in range(kvl):
            if r:
                z_copies[h, r].wait()
                relay(r, h, xbuf.at[0, r, :, pl.ds(h * hw, hw)])
            else:
                own_copies[h].wait()
        w_copy(r).wait()
        square = square + squares(0, r)
        x = xbuf[0, r]
        if r < E - 1:
            def body(i, carry, r=r, x=x):
                cols = pl.ds(pl.multiple_of(i * tile, tile), tile)
                part = dot(x, wbuf[r, :, cols])
                if r == 0:
                    acc[:, cols] = part
                else:
                    acc[:, cols] += part
                return carry

            lax.fori_loop(0, ff // tile, body, 0)
        else:
            def last(cols, r=r, x=x):
                part = dot(x, wbuf[r, :, cols])
                return part + acc[:, cols] if r else part

            give_back(0, square, last)
    for g in range(1, S):
        square = jnp.zeros((RB, 1), F32)
        for r in range(E):
            for h in range(kvl):
                x_copies[h, r, S - g].wait_recv()
            square = square + squares(g, r)

        def whole(cols, g=g):
            part = dot(xbuf[g, 0], wbuf[0, :, cols])
            for r in range(1, E):
                part = part + dot(xbuf[g, r], wbuf[r, :, cols])
            return part

        give_back(g, square, whole)
    for c in x_copies.values():
        c.wait_send()

    g0, g1 = column(gates_ref[0:1, :]), column(gates_ref[1:2, :])
    outs = []
    for g in range(S):
        base = pl.multiple_of(lax.rem(s + g, S) * ff, 128)
        for st, (c0, n) in enumerate(steps):
            for de in range(E):
                if g or de:
                    sends[st, de, g].wait()
            got = recv[g, :, :, c0:c0 + n].reshape(E * RP, n)
            res = dot(pick, got)
            for f in range(F):
                lo = 2 * f * T
                mix = g0 * res[lo:lo + T] + g1 * res[lo + T:lo + 2 * T]
                cols = slice(f * nc + c0, f * nc + c0 + n)
                out_ref[g, :, cols] = mix.astype(BF16)
        c = pltpu.make_async_copy(out_ref.at[g], out_hbm.at[:, pl.ds(base, ff)], out_sem.at[g])
        c.start()
        outs.append(c)
    for c in outs:
        c.wait()


def shards(queries, keys, values, lengths, routes, gates, w_up):
    S, E = lax.axis_size("seq"), lax.axis_size("expert")
    q_rows, width = queries.shape
    shard = keys.shape[0]
    w = w_up.reshape(w_up.shape[1], w_up.shape[2])
    depth, ff = w.shape
    T = routes.shape[0]
    cap = max(2, 3 * q_rows // (E * E))
    RB = up(E * cap, 16)
    choices = [f for f in range(1, ff // 128 + 1) if ff % (f * 128) == 0]
    F = min(choices, key=lambda f: up(f * cap, 16) * (ff // f))
    RP = up(F * cap, 16)
    nc = ff // F
    cuts = list(range(0, max(nc - 255, 1), 256))
    steps = [(c, (cuts + [nc])[i + 1] - c) for i, c in enumerate(cuts)]
    tile = 512 if ff % 512 == 0 else 128
    window = shard * S // 2
    pieces = []
    for d in range(1, S):
        first = max(0, (d + 1) * shard - q_rows - window + 1) // 16 * 16
        if first < shard:
            pieces.append((d, first))
    kv_rows = sum(shard - first for _, first in pieces)
    cfg = (S, E, lengths.shape[0], cap, RB, F, RP, nc, steps, pieces, tile)
    kvl = keys.shape[1] // HD
    dma = pltpu.SemaphoreType.DMA
    return pl.pallas_call(
        functools.partial(kernel, cfg),
        out_shape=jax.ShapeDtypeStruct((T, S * ff), BF16),
        in_specs=[pl.BlockSpec(memory_space=pl.ANY)] * 7,
        out_specs=pl.BlockSpec(memory_space=pl.ANY),
        scratch_shapes=[
            pltpu.SMEM(lengths.shape, jnp.int32),
            pltpu.VMEM(queries.shape, BF16),
            pltpu.VMEM(keys.shape, BF16),
            pltpu.VMEM(values.shape, BF16),
            pltpu.VMEM((2, T), jnp.int32),
            pltpu.VMEM((2, T), F32),
            pltpu.VMEM((S, T, ff), BF16),
            pltpu.VMEM((E, width, ff), BF16),
            pltpu.VMEM((kv_rows, keys.shape[1]), BF16),
            pltpu.VMEM((kv_rows, keys.shape[1]), BF16),
            pltpu.VMEM((E, 2, T), jnp.int32),
            pltpu.VMEM((E, RB, width), BF16),
            pltpu.VMEM((S, E, RB, width), BF16),
            pltpu.VMEM((RB, ff), F32),
            pltpu.VMEM((E, S, RP, nc), BF16),
            pltpu.VMEM((S, E, RP, nc), BF16),
            dma((6,)),
            dma((E,)),
            dma((2 * len(pieces),)),
            dma((2 * len(pieces),)),
            dma((E,)), dma((E,)), dma((kvl, E)), dma((kvl, E)),
            dma((kvl, E, S)), dma((kvl, E, S)),
            dma((kvl,)),
            dma((len(steps), E, S)), dma((len(steps), E, S)),
            dma((S,)),
        ],
        compiler_params=pltpu.CompilerParams(
            collective_id=0, has_side_effects=True, vmem_limit_bytes=60 * 1024 * 1024
        ),
    )(lengths, queries, keys, values, routes.T, gates.T, w)


def solution(mesh):
    placed = (
        P(("dp", "seq"), "expert"),
        P(("dp", "seq"), "expert"),
        P(("dp", "seq"), "expert"),
        P("dp"),
        P(("dp", "seq", "expert"), None),
        P(("dp", "seq", "expert"), None),
        P("expert", None, "seq"),
    )
    return jax.shard_map(
        shards,
        mesh=mesh,
        in_specs=placed,
        out_specs=P(("dp", "seq", "expert"), None),
        check_vma=False,
    )
```
